8 devices in a mesh: dp: 2 (over z, y), ep: 4 (over x, core).
Axes of the slice: x: 2, y: 2, z: 1, core: 2. Of those that a mesh axis runs over, the one named last changes fastest.
Arguments:
- x_in: bfloat16 [256, 384], P(('dp', 'ep')), parts along dimension 0
- idx_a: int32 [256, 6], P(('dp', 'ep')), parts along dimension 0
- idx_b: int32 [256, 6], P(('dp', 'ep')), parts along dimension 0
- gate_a: float32 [256, 6], P(('dp', 'ep')), parts along dimension 0
- gate_b: float32 [256, 6], P(('dp', 'ep')), parts along dimension 0
- dy_out: bfloat16 [256, 384], P(('dp', 'ep')), parts along dimension 0
- w1_a: bfloat16 [64, 384, 256], P('ep')
- w3_a: bfloat16 [64, 384, 256], P('ep')
- w2_a: bfloat16 [64, 256, 384], P('ep')
- w1_b: bfloat16 [64, 384, 256], P('ep')
- w3_b: bfloat16 [64, 384, 256], P('ep')
- w2_b: bfloat16 [64, 256, 384], P('ep')
Outputs:
- output 1: bfloat16 [256, 384], P(('dp', 'ep')), parts along dimension 0
- output 2: bfloat16 [256, 384], P(('dp', 'ep')), parts along dimension 0
- output 3: float32 [128, 384, 256], P(('dp', 'ep')), parts along dimension 0
- output 4: float32 [128, 384, 256], P(('dp', 'ep')), parts along dimension 0
- output 5: float32 [128, 256, 384], P(('dp', 'ep')), parts along dimension 0
- output 6: float32 [128, 384, 256], P(('dp', 'ep')), parts along dimension 0
- output 7: float32 [128, 384, 256], P(('dp', 'ep')), parts along dimension 0
- output 8: float32 [128, 256, 384], P(('dp', 'ep')), parts along dimension 0
- output 9: float32 [256, 6], P(('dp', 'ep')), parts along dimension 0
- output 10: float32 [256, 6], P(('dp', 'ep')), parts along dimension 0
There are 2 independent parts. The reference program is written for one: setup_inputs(seed, part) draws one part's arguments, and reference() takes and returns one part's arrays. A program takes and returns all parts, laid end to end along the dimension named above; an argument that names none is the same for every part.
All inputs are finite; a program needn't handle non-finite values.
Results may differ from the reference program's by a relative error of at most 0.00583839.
Values are sent between devices in bfloat16 or wider.
A program may use at most 1 GiB of HBM per device.

```python
import jax
import jax.numpy as jnp
from jax import lax

TOKENS = 32
D = 384
FF = 256
EXPERTS = 64
TOP = 6
GROUP = 4
CAP = 12
HOT = 4


def draw_routing(root_key):
    key_hot, key_dev = jax.random.split(root_key)
    ranking = jax.random.permutation(key_hot, EXPERTS)
    cold_total = EXPERTS - HOT
    spare_pairs = TOKENS * TOP - HOT * CAP
    base_count = spare_pairs // cold_total
    extra_count = spare_pairs - base_count * cold_total

    def one_device(dev_key):
        key_count, key_rows, key_shift = jax.random.split(dev_key, 3)
        cold_rank = jax.random.permutation(key_count, cold_total)
        cold_count = base_count + (cold_rank < extra_count).astype(jnp.int32)
        by_rank = jnp.concatenate([jnp.full((HOT,), CAP, jnp.int32), cold_count])
        expert_count = jnp.zeros((EXPERTS,), jnp.int32).at[ranking].set(by_rank)
        run_ends = jnp.cumsum(expert_count)
        positions = jnp.arange(TOKENS * TOP, dtype=jnp.int32)
        sorted_ids = jnp.searchsorted(run_ends, positions, side="right").astype(jnp.int32)
        id_table = sorted_ids.reshape(TOP, TOKENS).T
        id_table = id_table[jax.random.permutation(key_rows, TOKENS)]
        row_shift = jax.random.randint(key_shift, (TOKENS, 1), 0, TOP)
        col_order = (jnp.arange(TOP)[None, :] + row_shift) % TOP
        return jnp.take_along_axis(id_table, col_order, axis=1)

    return jax.vmap(one_device)(jax.random.split(key_dev, GROUP)).reshape(GROUP * TOKENS, TOP)


def setup_inputs(seed: int = 0, part: int = 0) -> dict:
    root_key = jax.random.key(seed)
    shared_keys = jax.random.split(root_key, 6)
    part_keys = jax.random.split(jax.random.fold_in(root_key, part), 6)
    row_total = GROUP * TOKENS
    gate_scale = 1.5 / TOP ** 0.5
    in_scale = D ** -0.5
    mid_scale = FF ** -0.5
    x_in = jax.random.normal(part_keys[0], (row_total, D), jnp.float32).astype(jnp.bfloat16)
    idx_a = draw_routing(part_keys[1])
    idx_b = draw_routing(part_keys[2])
    gate_a = (0.5 + jax.random.uniform(part_keys[3], (row_total, TOP), jnp.float32)) * gate_scale
    gate_b = (0.5 + jax.random.uniform(part_keys[4], (row_total, TOP), jnp.float32)) * gate_scale
    dy_out = jax.random.normal(part_keys[5], (row_total, D), jnp.float32).astype(jnp.bfloat16)
    w1_a = (jax.random.normal(shared_keys[0], (EXPERTS, D, FF), jnp.float32) * in_scale).astype(jnp.bfloat16)
    w3_a = (jax.random.normal(shared_keys[1], (EXPERTS, D, FF), jnp.float32) * in_scale).astype(jnp.bfloat16)
    w2_a = (jax.random.normal(shared_keys[2], (EXPERTS, FF, D), jnp.float32) * mid_scale).astype(jnp.bfloat16)
    w1_b = (jax.random.normal(shared_keys[3], (EXPERTS, D, FF), jnp.float32) * in_scale).astype(jnp.bfloat16)
    w3_b = (jax.random.normal(shared_keys[4], (EXPERTS, D, FF), jnp.float32) * in_scale).astype(jnp.bfloat16)
    w2_b = (jax.random.normal(shared_keys[5], (EXPERTS, FF, D), jnp.float32) * mid_scale).astype(jnp.bfloat16)
    return {"x_in": x_in, "idx_a": idx_a, "idx_b": idx_b, "gate_a": gate_a, "gate_b": gate_b, "dy_out": dy_out, "w1_a": w1_a, "w3_a": w3_a, "w2_a": w2_a, "w1_b": w1_b, "w3_b": w3_b, "w2_b": w2_b}


def expert_forward(u_rows, w_gate, w_up, w_down):
    pre_gate = jnp.dot(u_rows, w_gate, preferred_element_type=jnp.float32)
    pre_up = jnp.dot(u_rows, w_up, preferred_element_type=jnp.float32)
    hidden = (jax.nn.silu(pre_gate) * pre_up).astype(jnp.bfloat16)
    out_rows = jnp.dot(hidden, w_down, preferred_element_type=jnp.float32).astype(jnp.bfloat16)
    return pre_gate, pre_up, hidden, out_rows


def device_slots(flat_ids):
    onehot = (flat_ids[:, None] == jnp.arange(EXPERTS, dtype=jnp.int32)[None, :]).astype(jnp.int32)
    return jnp.sum(jnp.cumsum(onehot, axis=0) * onehot, axis=1) - 1


def expert_table(ids):
    per_device = ids.reshape(GROUP, TOKENS * TOP)
    pair_slot = lax.map(device_slots, per_device)
    expert_row = jnp.arange(GROUP, dtype=jnp.int32)[:, None] * CAP + pair_slot
    pair_ids = jnp.arange(GROUP * TOKENS * TOP, dtype=jnp.int32).reshape(GROUP, TOKENS * TOP)
    empty_pair = GROUP * TOKENS * TOP
    return jnp.full((EXPERTS, GROUP * CAP), empty_pair, jnp.int32).at[per_device, expert_row].set(pair_ids)


def layer_forward(x_rows, gates, table, w_gate, w_up, w_down):
    x_pad = jnp.concatenate([x_rows, jnp.zeros((1, D), x_rows.dtype)])
    gate_pad = jnp.concatenate([gates.reshape(-1), jnp.zeros((1,), gates.dtype)])

    def expert_step(out_acc, step_in):
        pair_ids, gate_w, up_w, down_w = step_in
        tok_index = pair_ids // TOP
        out_rows = expert_forward(x_pad[tok_index], gate_w, up_w, down_w)[3]
        weighted = gate_pad[pair_ids][:, None] * out_rows.astype(jnp.float32)
        return out_acc.at[tok_index].add(weighted), None

    out_acc = jnp.zeros((GROUP * TOKENS + 1, D), jnp.float32)
    out_acc = lax.scan(expert_step, out_acc, (table, w_gate, w_up, w_down))[0]
    return (x_rows.astype(jnp.float32) + out_acc[:-1]).astype(jnp.bfloat16)


def layer_backward(dy_rows, x_rows, gates, table, w_gate, w_up, w_down):
    x_pad = jnp.concatenate([x_rows, jnp.zeros((1, D), x_rows.dtype)])
    dy_pad = jnp.concatenate([dy_rows, jnp.zeros((1, D), dy_rows.dtype)])
    gate_pad = jnp.concatenate([gates.reshape(-1), jnp.zeros((1,), gates.dtype)])

    def expert_step(carry_in, step_in):
        dx_acc, dgate_acc = carry_in
        pair_ids, gate_w, up_w, down_w = step_in
        tok_index = pair_ids // TOP
        u_rows = x_pad[tok_index]
        dy_exp = dy_pad[tok_index].astype(jnp.float32)
        pre_gate, pre_up, hidden, out_rows = expert_forward(u_rows, gate_w, up_w, down_w)
        dgate_rows = jnp.sum(dy_exp * out_rows.astype(jnp.float32), axis=1)
        d_out = (gate_pad[pair_ids][:, None] * dy_exp).astype(jnp.bfloat16)
        dw_down = jnp.dot(hidden.T, d_out, preferred_element_type=jnp.float32)
        d_hidden = jnp.dot(d_out, down_w.T, preferred_element_type=jnp.float32)
        gate_sig = jax.nn.sigmoid(pre_gate)
        d_pre_gate = (d_hidden * pre_up * gate_sig * (1.0 + pre_gate * (1.0 - gate_sig))).astype(jnp.bfloat16)
        d_pre_up = (d_hidden * jax.nn.silu(pre_gate)).astype(jnp.bfloat16)
        dw_gate = jnp.dot(u_rows.T, d_pre_gate, preferred_element_type=jnp.float32)
        dw_up = jnp.dot(u_rows.T, d_pre_up, preferred_element_type=jnp.float32)
        du_rows = (jnp.dot(d_pre_gate, gate_w.T, preferred_element_type=jnp.float32) + jnp.dot(d_pre_up, up_w.T, preferred_element_type=jnp.float32)).astype(jnp.bfloat16)
        dx_acc = dx_acc.at[tok_index].add(du_rows.astype(jnp.float32))
        dgate_acc = dgate_acc.at[pair_ids].set(dgate_rows)
        return (dx_acc, dgate_acc), (dw_gate, dw_up, dw_down)

    dx_acc = jnp.zeros((GROUP * TOKENS + 1, D), jnp.float32)
    dgate_acc = jnp.zeros((GROUP * TOKENS * TOP + 1,), jnp.float32)
    (dx_acc, dgate_acc), grads = lax.scan(expert_step, (dx_acc, dgate_acc), (table, w_gate, w_up, w_down))
    dx_rows = (dy_rows.astype(jnp.float32) + dx_acc[:-1]).astype(jnp.bfloat16)
    return dx_rows, dgate_acc[:-1].reshape(GROUP * TOKENS, TOP), grads


def reference(x_in, idx_a, idx_b, gate_a, gate_b, dy_out, w1_a, w3_a, w2_a, w1_b, w3_b, w2_b):
    table_a = expert_table(idx_a)
    table_b = expert_table(idx_b)
    x_mid = layer_forward(x_in, gate_a, table_a, w1_a, w3_a, w2_a)
    x_out = layer_forward(x_mid, gate_b, table_b, w1_b, w3_b, w2_b)
    dx_mid, dgate_b, grads_b = layer_backward(dy_out, x_mid, gate_b, table_b, w1_b, w3_b, w2_b)
    dx_in, dgate_a, grads_a = layer_backward(dx_mid, x_in, gate_a, table_a, w1_a, w3_a, w2_a)
    return (x_out, dx_in, grads_a[0], grads_a[1], grads_a[2], grads_b[0], grads_b[1], grads_b[2], dgate_a, dgate_b)
```

```python
import functools

import jax
import jax.numpy as jnp
from jax import lax
from jax.experimental import pallas as pl
from jax.experimental.pallas import tpu as pltpu
from jax.sharding import PartitionSpec as P

MESH = pl.DeviceIdType.MESH
F32 = jnp.float32
BF16 = jnp.bfloat16
NN = (((1,), (0,)), ((), ()))
NT = (((1,), (1,)), ((), ()))
TN = (((0,), (0,)), ((), ()))
LANES = 128
PAD = 8


def mm(lhs, rhs, dims=NN):
    return lax.dot_general(lhs, rhs, dims, preferred_element_type=F32)


def step_kernel(
    n, x_ref, dy_ref, idx_a_ref, idx_b_ref, gate_a_ref, gate_b_ref,
    w1_a, w3_a, w2_a, w1_b, w3_b, w2_b,
    x_out_ref, dx_in_ref, dgate_a_ref, dgate_b_ref, xg_a, xg_b, dyg_a, dyg_b, ids_ref, gates_ref, h_out, da_out, db_out,
    w1_v, w3_v, w2_v, h_v, da_v, db_v, planes, meta, meta_own, acc, acc_fwd, recv, own, dg, dg_send, dg_recv, xg_first,
    w_sem, f_sem, send_sem, recv_sem,
):
    local_experts = w1_a.shape[0]
    tok = x_ref.shape[0]
    width = x_ref.shape[1]
    top = idx_a_ref.shape[1]
    rows = n * tok
    me = lax.axis_index("ep")
    first_expert = me * local_experts
    weights = ((w1_a, w3_a, w2_a), (w1_b, w3_b, w2_b))
    slots = (w1_v, w3_v, w2_v)

    def weight_copy(layer, kind, e):
        return pltpu.make_async_copy(weights[layer][kind].at[e], slots[kind].at[layer, e], w_sem.at[layer, kind, e])

    for layer in range(2):
        for kind in range(3):
            @pl.loop(0, local_experts)
            def _(e):
                weight_copy(layer, kind, e).start()

    barrier = pltpu.get_barrier_semaphore()
    for k in range(1, n):
        pl.semaphore_signal(barrier, inc=1, device_id={"ep": lax.rem(me + k, n)}, device_id_type=MESH)
    pl.semaphore_wait(barrier, n - 1)

    def exchange(event, source, target):
        copies = []
        for k in (2, 1, 3):
            peer = lax.rem(me + k, n)
            copy = pltpu.make_async_remote_copy(
                src_ref=source(peer), dst_ref=target.at[me], send_sem=send_sem.at[event, k - 1], recv_sem=recv_sem.at[event, k - 1],
                device_id={"ep": peer}, device_id_type=MESH)
            copy.start()
            copies.append(copy)
        return copies

    def wait(copies):
        for copy in copies:
            copy.wait()

    first_x = exchange(0, lambda peer: x_ref, xg_first)
    xg_first[me] = x_ref[...]

    planes[...] = jnp.full_like(planes, -1.0)
    planes[0, :, 0:top] = idx_a_ref[...].astype(F32)
    planes[1, :, 0:top] = idx_b_ref[...].astype(F32)
    planes[2, :, 0:top] = gate_a_ref[...]
    planes[3, :, 0:top] = gate_b_ref[...]
    lane = lax.broadcasted_iota(jnp.int32, (tok, LANES), 1)
    packed = planes[0]
    for p in range(1, 4):
        packed = jnp.where(lane < p * PAD, packed, pltpu.roll(planes[p], p * PAD, 1))
    meta_own[...] = packed
    meta[me] = packed
    sent_meta = exchange(1, lambda peer: meta_own, meta)
    sent_dy = exchange(2, lambda peer: dy_ref, dyg_b)
    dyg_b[me] = dy_ref[...]

    def flat(ref):
        value = ref[...]
        return value.reshape(value.shape[0] * value.shape[1], value.shape[2])

    def pair_gate(layer, e):
        hit = ids_ref[layer] == (first_expert + e).astype(F32)
        gate = jnp.sum(jnp.where(hit, gates_ref[layer], 0.0), axis=1, keepdims=True)
        return hit, gate

    def hidden_of(layer, e, u_rows):
        pre_gate = mm(u_rows, w1_v[layer, e])
        pre_up = mm(u_rows, w3_v[layer, e])
        sig = jax.nn.sigmoid(pre_gate)
        silu = pre_gate * sig
        return pre_gate, pre_up, sig, silu, (silu * pre_up).astype(BF16)

    def add_rows(total, value):
        total[...] += value.reshape(total.shape)

    def forward(layer, u_ref, total, wait_weights):
        total[...] = jnp.zeros_like(total)
        u_rows = flat(u_ref)

        @pl.loop(0, local_experts)
        def _(e):
            if wait_weights:
                weight_copy(layer, 0, e).wait()
                weight_copy(layer, 1, e).wait()
            h_v[layer, e] = hidden_of(layer, e, u_rows)[4]

        if wait_weights:
            wait(sent_meta)
            all_meta = flat(meta)
            wide_lane = lax.broadcasted_iota(jnp.int32, (rows, LANES), 1)
            for which in range(2):
                ids = pltpu.roll(all_meta, LANES - which * PAD, 1) if which else all_meta
                ids_ref[which] = jnp.where(wide_lane < top, ids, -1.0)
                gates_ref[which] = pltpu.roll(all_meta, LANES - (2 + which) * PAD, 1)

        @pl.loop(0, local_experts)
        def _(e):
            if wait_weights:
                weight_copy(layer, 2, e).wait()
            gate = pair_gate(layer, e)[1]
            out_rows = mm(h_v[layer, e], w2_v[layer, e]).astype(BF16).astype(F32)
            add_rows(total, jnp.where(gate > 0.0, gate * out_rows, 0.0))

    def factor_copies(layer, e):
        return [pltpu.make_async_copy(v.at[layer, e], o.at[layer, e], f_sem.at[layer, i, e])
                for i, (v, o) in enumerate(((h_v, h_out), (da_v, da_out), (db_v, db_out)))]

    def backward(layer, u_ref, dy_all_ref, total):
        total[...] = jnp.zeros_like(total)
        dg[layer] = jnp.zeros_like(dg[layer])
        u_rows = flat(u_ref)
        dy_rows = flat(dy_all_ref)

        @pl.loop(0, local_experts)
        def _(e):
            pre_gate, pre_up, sig, silu, hidden = hidden_of(layer, e, u_rows)
            hit, gate = pair_gate(layer, e)
            live = gate > 0.0
            wide = dy_rows.astype(F32)
            q = (gate * wide).astype(BF16)
            d_hidden = mm(q, w2_v[layer, e], NT)
            d_gate = jnp.where(live, d_hidden * pre_up * sig * (1.0 + pre_gate * (1.0 - sig)), 0.0).astype(BF16)
            d_up = jnp.where(live, d_hidden * silu, 0.0).astype(BF16)
            du = mm(d_gate, w1_v[layer, e], NT) + mm(d_up, w3_v[layer, e], NT)
            add_rows(total, du.astype(BF16).astype(F32))
            out_rows = mm(hidden, w2_v[layer, e]).astype(BF16).astype(F32)
            dgate_col = jnp.sum(wide * out_rows, axis=1, keepdims=True)
            dg[layer] += jnp.where(hit, dgate_col, 0.0)
            h_v[layer, e] = jnp.where(live, hidden.astype(F32), 0.0).astype(BF16)
            da_v[layer, e] = d_gate
            db_v[layer, e] = d_up
            for copy in factor_copies(layer, e):
                copy.start()

    def finish_factors(layer):
        @pl.loop(0, local_experts)
        def _(e):
            for copy in factor_copies(layer, e):
                copy.wait()

    def reduced(event, base, total):
        value = base.astype(F32) + total[me]
        for k in range(1, n):
            value += recv[event, lax.rem(me + k, n)]
        return value.astype(BF16)

    wait(first_x)
    forward(0, xg_first, acc, True)
    sent = exchange(3, lambda peer: acc.at[peer], recv.at[0])
    wait(sent)
    x_mid = reduced(0, x_ref[...], acc)
    own[0] = x_mid
    xg_b[me] = x_mid
    sent_mid = exchange(4, lambda peer: own.at[0], xg_b)

    @pl.loop(0, local_experts)
    def _(e):
        for kind in range(3):
            weight_copy(1, kind, e).wait()

    wait(sent_dy)
    wait(sent_mid)
    again = exchange(5, lambda peer: x_ref, xg_a)
    xg_a[me] = x_ref[...]

    backward(1, xg_b, dyg_b, acc)
    sent = exchange(6, lambda peer: acc.at[peer], recv.at[1])
    finish_factors(1)
    h_keep = None
    del h_keep
    forward(1, xg_b, acc_fwd, False)
    sent_out = exchange(7, lambda peer: acc_fwd.at[peer], recv.at[2])
    wait(sent)
    dx_mid = reduced(1, dy_ref[...], acc)
    own[1] = dx_mid
    dyg_a[me] = dx_mid
    sent_mid = exchange(8, lambda peer: own.at[1], dyg_a)
    wait(sent_out)
    x_out_ref[...] = reduced(2, own[0], acc_fwd)
    wait(again)
    wait(sent_mid)

    backward(0, xg_a, dyg_a, acc)
    sent = exchange(9, lambda peer: acc.at[peer], recv.at[3])
    both = jnp.where(lax.broadcasted_iota(jnp.int32, (rows, LANES), 1) < PAD, dg[0], pltpu.roll(dg[1], PAD, 1))
    dg_send[...] = both.reshape(dg_send.shape)
    sent_dg = exchange(10, lambda peer: dg_send.at[peer], dg_recv)
    finish_factors(0)
    wait(sent)
    dx_in_ref[...] = reduced(3, dy_ref[...] if False else own[1], acc)
    wait(sent_dg)
    value = dg_send[me]
    for k in range(1, n):
        value += dg_recv[lax.rem(me + k, n)]
    dgate_a_ref[...] = value[:, 0:top]
    dgate_b_ref[...] = pltpu.roll(value, LANES - PAD, 1)[:, 0:top]


def grads_kernel(
    xa, xb, dya, dyb, ids_ref, gates_ref, h_ref, da_ref, db_ref, x_out_in, dx_in_in, dga_in, dgb_in,
    dw1_a, dw3_a, dw2_a, dw1_b, dw3_b, dw2_b, x_out, dx_in, dga, dgb,
):
    e = pl.program_id(0)
    expert = lax.axis_index("ep") * pl.num_programs(0) + e

    @pl.when(e == 0)
    def _():
        x_out[...] = x_out_in[...]
        dx_in[...] = dx_in_in[...]
        dga[...] = dga_in[...]
        dgb[...] = dgb_in[...]

    for layer, (x, dy, dw1, dw3, dw2) in enumerate(((xa, dya, dw1_a, dw3_a, dw2_a), (xb, dyb, dw1_b, dw3_b, dw2_b))):
        gate = jnp.sum(jnp.where(ids_ref[layer] == expert.astype(F32), gates_ref[layer], 0.0), axis=1, keepdims=True)
        q = (gate * dy[...].astype(F32)).astype(BF16)
        dw2[0] = mm(h_ref[layer, 0], q, TN)
        dw1[0] = mm(x[...], da_ref[layer, 0], TN)
        dw3[0] = mm(x[...], db_ref[layer, 0], TN)


def solution(mesh):
    n = mesh.shape["ep"]
    tok_spec = P(("dp", "ep"))
    w_spec = P("ep")

    def device_program(x_in, idx_a, idx_b, gate_a, gate_b, dy_out, w1_a, w3_a, w2_a, w1_b, w3_b, w2_b):
        tok, width = x_in.shape
        top = idx_a.shape[1]
        experts, _, ff = w1_a.shape
        rows = n * tok
        vmem = pl.BlockSpec(memory_space=pltpu.VMEM)
        anyw = pl.BlockSpec(memory_space=pl.ANY)
        sds = jax.ShapeDtypeStruct
        factor = sds((2, experts, rows, ff), BF16)
        gathered = sds((n, tok, width), BF16)
        outs = pl.pallas_call(
            functools.partial(step_kernel, n),
            out_shape=(
                sds((tok, width), BF16), sds((tok, width), BF16), sds((tok, top), F32), sds((tok, top), F32),
                gathered, gathered, gathered, gathered,
                sds((2, rows, LANES), F32), sds((2, rows, LANES), F32), factor, factor, factor),
            in_specs=[vmem] * 6 + [anyw] * 6,
            out_specs=(vmem,) * 10 + (anyw,) * 3,
            scratch_shapes=[
                pltpu.VMEM((2, experts, width, ff), BF16), pltpu.VMEM((2, experts, width, ff), BF16), pltpu.VMEM((2, experts, ff, width), BF16),
                pltpu.VMEM((2, experts, rows, ff), BF16), pltpu.VMEM((2, experts, rows, ff), BF16), pltpu.VMEM((2, experts, rows, ff), BF16),
                pltpu.VMEM((4, tok, LANES), F32), pltpu.VMEM((n, tok, LANES), F32), pltpu.VMEM((tok, LANES), F32),
                pltpu.VMEM((n, tok, width), F32), pltpu.VMEM((n, tok, width), F32), pltpu.VMEM((4, n, tok, width), F32), pltpu.VMEM((2, tok, width), BF16),
                pltpu.VMEM((2, rows, LANES), F32), pltpu.VMEM((n, tok, LANES), F32), pltpu.VMEM((n, tok, LANES), F32),
                pltpu.VMEM((n, tok, width), BF16),
                pltpu.SemaphoreType.DMA((2, 3, experts)), pltpu.SemaphoreType.DMA((2, 3, experts)),
                pltpu.SemaphoreType.DMA((11, n - 1)), pltpu.SemaphoreType.DMA((11, n - 1)),
            ],
            compiler_params=pltpu.CompilerParams(collective_id=0, has_side_effects=True, vmem_limit_bytes=56 << 20),
            name="moe_step",
        )(x_in, dy_out, idx_a, idx_b, gate_a, gate_b, w1_a, w3_a, w2_a, w1_b, w3_b, w2_b)
        x_out, dx_in, dga, dgb, xa, xb, dya, dyb, ids, gates, h, da, db = outs
        flat = lambda v: v.reshape(rows, width)
        whole = lambda v: pl.BlockSpec(v.shape, lambda e: (0,) * v.ndim)
        fac = pl.BlockSpec((2, 1, rows, ff), lambda e: (0, e, 0, 0))
        dw_up = pl.BlockSpec((1, width, ff), lambda e: (e, 0, 0))
        dw_down = pl.BlockSpec((1, ff, width), lambda e: (e, 0, 0))
        small = [flat(xa), flat(xb), flat(dya), flat(dyb), ids, gates]
        last = [x_out, dx_in, dga, dgb]
        up, down = sds((experts, width, ff), F32), sds((experts, ff, width), F32)
        res = pl.pallas_call(
            grads_kernel,
            grid=(experts,),
            out_shape=(up, up, down, up, up, down) + tuple(sds(v.shape, v.dtype) for v in last),
            in_specs=[whole(v) for v in small] + [fac] * 3 + [whole(v) for v in last],
            out_specs=(dw_up, dw_up, dw_down, dw_up, dw_up, dw_down) + tuple(whole(v) for v in last),
            compiler_params=pltpu.CompilerParams(dimension_semantics=("arbitrary",), vmem_limit_bytes=32 << 20),
            name="moe_grads",
        )(*small, h, da, db, *last)
        g = res[:6]
        x_out, dx_in, dga, dgb = res[6:]
        return (x_out, dx_in) + g + (dga, dgb)

    return jax.shard_map(device_program, mesh=mesh, in_specs=(tok_spec,) * 6 + (w_spec,) * 6, out_specs=(tok_spec,) * 10, check_vma=False)
```

```python
import functools

import jax
import jax.numpy as jnp
from jax import lax
from jax.experimental import pallas as pl
from jax.experimental.pallas import tpu as pltpu
from jax.sharding import PartitionSpec as P

MESH = pl.DeviceIdType.MESH
F32 = jnp.float32
BF16 = jnp.bfloat16
NN = (((1,), (0,)), ((), ()))
NT = (((1,), (1,)), ((), ()))
TN = (((0,), (0,)), ((), ()))
LANES = 128
PAD = 8


def mm(lhs, rhs, dims=NN):
    return lax.dot_general(lhs, rhs, dims, preferred_element_type=F32)


def step_kernel(
    n, x_ref, dy_ref, idx_a_ref, idx_b_ref, gate_a_ref, gate_b_ref,
    w1_a, w3_a, w2_a, w1_b, w3_b, w2_b,
    x_out_ref, dx_in_ref, dgate_a_ref, dgate_b_ref, xa_out, xb_out, dya_out, dyb_out, ids_out, gates_out, h_out, da_out, db_out,
    w1_v, w3_v, w2_v, h_v, da_v, db_v, hf_v, dh_v, slope_v, silu_v,
    planes, meta, meta_own, square, ids_ref, gates_ref, xg_first, xg_a, xg_b, dyg_a, dyg_b,
    acc, acc_fwd, recv, own, dg, dg_send, dg_recv,
    w_sem, f_sem, o_sem, send_sem, recv_sem,
):
    local_experts = w1_a.shape[0]
    tok = x_ref.shape[0]
    top = idx_a_ref.shape[0]
    rows = n * tok
    me = lax.axis_index("ep")
    first_expert = me * local_experts
    weights = ((w1_a, w3_a, w2_a), (w1_b, w3_b, w2_b))
    slots = (w1_v, w3_v, w2_v)

    def weight_copy(layer, kind, e):
        return pltpu.make_async_copy(weights[layer][kind].at[e], slots[kind].at[layer, e], w_sem.at[layer, kind, e])

    for layer in range(2):
        for kind in range(3):
            @pl.loop(0, local_experts)
            def _(e):
                weight_copy(layer, kind, e).start()

    barrier = pltpu.get_barrier_semaphore()
    for k in range(1, n):
        pl.semaphore_signal(barrier, inc=1, device_id={"ep": lax.rem(me + k, n)}, device_id_type=MESH)
    pl.semaphore_wait(barrier, n - 1)

    def exchange(event, source, target):
        copies = []
        for k in (2, 1, 3):
            peer = lax.rem(me + k, n)
            copy = pltpu.make_async_remote_copy(
                src_ref=source(peer), dst_ref=target.at[me], send_sem=send_sem.at[event, k - 1], recv_sem=recv_sem.at[event, k - 1],
                device_id={"ep": peer}, device_id_type=MESH)
            copy.start()
            copies.append(copy)
        return copies

    def wait(copies):
        for copy in copies:
            copy.wait()

    first_x = exchange(0, lambda peer: x_ref, xg_first)
    xg_first[me] = x_ref[...]

    planes[...] = jnp.full_like(planes, -1.0)
    planes[0, 0:top, 0:tok] = idx_a_ref[...].astype(F32)
    planes[1, 0:top, 0:tok] = idx_b_ref[...].astype(F32)
    planes[2, 0:top, 0:tok] = gate_a_ref[...]
    planes[3, 0:top, 0:tok] = gate_b_ref[...]
    lane = lax.broadcasted_iota(jnp.int32, (PAD, LANES), 1)
    packed = planes[0]
    for p in range(1, 4):
        packed = jnp.where(lane < p * tok, packed, pltpu.roll(planes[p], p * tok, 1))
    meta_own[...] = packed
    meta[me] = packed
    sent_meta = exchange(1, lambda peer: meta_own, meta)
    sent_dy = exchange(2, lambda peer: dy_ref, dyg_b)
    dyg_b[me] = dy_ref[...]

    def read_meta():
        square[...] = jnp.full_like(square, -1.0)
        for kind in range(4):
            value = None
            for s in range(n):
                turned = pltpu.roll(meta[s], (s - kind) % n * tok, 1)
                value = turned if value is None else jnp.where(lane < s * tok, value, turned)
            square[kind * PAD:(kind + 1) * PAD, :] = value
        all_meta = square[...].T
        wide_lane = lax.broadcasted_iota(jnp.int32, (rows, LANES), 1)
        for layer in range(2):
            ids = pltpu.roll(all_meta, LANES - PAD, 1) if layer else all_meta
            ids_ref[layer] = jnp.where(wide_lane < top, ids, -1.0)
            gates_ref[layer] = pltpu.roll(all_meta, LANES - (2 + layer) * PAD, 1)

    def flat(ref):
        value = ref[...]
        return value.reshape(value.shape[0] * value.shape[1], value.shape[2])

    def pair_gate(layer, e):
        hit = ids_ref[layer] == (first_expert + e).astype(F32)
        gate = jnp.sum(jnp.where(hit, gates_ref[layer], 0.0), axis=1, keepdims=True)
        return hit, gate

    def hidden_of(layer, e, u_rows):
        pre_gate = mm(u_rows, w1_v[layer, e])
        pre_up = mm(u_rows, w3_v[layer, e])
        sig = jax.nn.sigmoid(pre_gate)
        silu = pre_gate * sig
        return pre_gate, pre_up, sig, silu, silu * pre_up

    def add_rows(total, value):
        total[...] += value.reshape(total.shape)

    def forward_hidden(layer, u_ref, first):
        u_rows = flat(u_ref)

        @pl.loop(0, local_experts)
        def _(e):
            if first:
                weight_copy(layer, 0, e).wait()
                weight_copy(layer, 1, e).wait()
            hf_v[e] = hidden_of(layer, e, u_rows)[4].astype(BF16)

    def forward_out(layer, total, first):
        total[...] = jnp.zeros_like(total)

        @pl.loop(0, local_experts)
        def _(e):
            if first:
                weight_copy(layer, 2, e).wait()
            gate = pair_gate(layer, e)[1]
            out_rows = mm(hf_v[e], w2_v[layer, e]).astype(BF16).astype(F32)
            add_rows(total, jnp.where(gate > 0.0, gate * out_rows, 0.0))

    def factor_copies(layer, e):
        return [pltpu.make_async_copy(v.at[layer, e], o.at[layer, e], f_sem.at[layer, i, e])
                for i, (v, o) in enumerate(((h_v, h_out), (da_v, da_out), (db_v, db_out)))]

    def d_hidden_of(layer, e, dy_rows, gate):
        q = (gate * dy_rows.astype(F32)).astype(BF16)
        return mm(q, w2_v[layer, e], NT)

    def put_back(layer, e, d_gate, d_up, total):
        da_v[layer, e] = d_gate
        db_v[layer, e] = d_up
        du = mm(d_gate, w1_v[layer, e], NT) + mm(d_up, w3_v[layer, e], NT)
        add_rows(total, du.astype(BF16).astype(F32))

    def gate_grads(layer, dy_all_ref):
        dg[layer] = jnp.zeros_like(dg[layer])
        dy_rows = flat(dy_all_ref)

        @pl.loop(0, local_experts)
        def _(e):
            hit = pair_gate(layer, e)[0]
            out_rows = mm(h_v[layer, e], w2_v[layer, e]).astype(BF16).astype(F32)
            dgate_col = jnp.sum(dy_rows.astype(F32) * out_rows, axis=1, keepdims=True)
            dg[layer] += jnp.where(hit, dgate_col, 0.0)

    def reduced(event, base, total):
        value = base.astype(F32) + total[me]
        for k in range(1, n):
            value += recv[event, lax.rem(me + k, n)]
        return value.astype(BF16)

    kept = ((xg_a, xa_out), (xg_b, xb_out), (dyg_a, dya_out), (dyg_b, dyb_out), (ids_ref, ids_out), (gates_ref, gates_out))

    def keep(*which):
        for i in which:
            pltpu.make_async_copy(kept[i][0], kept[i][1], o_sem.at[i]).start()

    wait(first_x)
    forward_hidden(0, xg_first, True)
    wait(sent_meta)
    read_meta()
    forward_out(0, acc, True)
    sent = exchange(3, lambda peer: acc.at[peer], recv.at[0])

    keep(4, 5)
    wait(sent_dy)
    keep(3)
    dy_b = flat(dyg_b)

    @pl.loop(0, local_experts)
    def _(e):
        weight_copy(1, 0, e).wait()
        weight_copy(1, 1, e).wait()
        weight_copy(1, 2, e).wait()
        dh_v[e] = d_hidden_of(1, e, dy_b, pair_gate(1, e)[1])

    wait(sent)
    x_mid = reduced(0, x_ref[...], acc)
    own[0] = x_mid
    xg_b[me] = x_mid
    sent_mid = exchange(4, lambda peer: own.at[0], xg_b)
    wait(sent_mid)
    keep(1)
    again = exchange(5, lambda peer: x_ref, xg_a)
    xg_a[me] = x_ref[...]

    acc[...] = jnp.zeros_like(acc)
    u_b = flat(xg_b)

    @pl.loop(0, local_experts)
    def _(e):
        pre_gate, pre_up, sig, silu, hidden = hidden_of(1, e, u_b)
        live = pair_gate(1, e)[1] > 0.0
        d_hidden = dh_v[e]
        d_gate = jnp.where(live, d_hidden * pre_up * sig * (1.0 + pre_gate * (1.0 - sig)), 0.0).astype(BF16)
        d_up = jnp.where(live, d_hidden * silu, 0.0).astype(BF16)
        h_v[1, e] = jnp.where(live, hidden, 0.0).astype(BF16)
        put_back(1, e, d_gate, d_up, acc)
        for copy in factor_copies(1, e):
            copy.start()

    sent = exchange(6, lambda peer: acc.at[peer], recv.at[1])

    gate_grads(1, dyg_b)
    forward_hidden(1, xg_b, False)
    forward_out(1, acc_fwd, False)
    wait(sent)
    dx_mid = reduced(1, dy_ref[...], acc)
    own[1] = dx_mid
    dyg_a[me] = dx_mid
    sent_mid = exchange(7, lambda peer: own.at[1], dyg_a)
    sent_out = exchange(8, lambda peer: acc_fwd.at[peer], recv.at[2])

    wait(again)
    keep(0)
    u_a = flat(xg_a)

    @pl.loop(0, local_experts)
    def _(e):
        pre_gate, pre_up, sig, silu, hidden = hidden_of(0, e, u_a)
        live = pair_gate(0, e)[1] > 0.0
        slope_v[e] = jnp.where(live, pre_up * sig * (1.0 + pre_gate * (1.0 - sig)), 0.0)
        silu_v[e] = jnp.where(live, silu, 0.0)
        h_v[0, e] = jnp.where(live, hidden, 0.0).astype(BF16)

    wait(sent_mid)
    keep(2)
    acc[...] = jnp.zeros_like(acc)
    dy_a = flat(dyg_a)

    @pl.loop(0, local_experts)
    def _(e):
        d_hidden = d_hidden_of(0, e, dy_a, pair_gate(0, e)[1])
        put_back(0, e, (d_hidden * slope_v[e]).astype(BF16), (d_hidden * silu_v[e]).astype(BF16), acc)
        for copy in factor_copies(0, e):
            copy.start()

    sent = exchange(9, lambda peer: acc.at[peer], recv.at[3])
    gate_grads(0, dyg_a)
    both = jnp.where(lax.broadcasted_iota(jnp.int32, (rows, LANES), 1) < PAD, dg[0], pltpu.roll(dg[1], PAD, 1)).T
    dg_send[...] = both[0:2 * PAD]
    sent_dg = exchange(10, lambda peer: dg_send, dg_recv)
    wait(sent_out)
    x_out_ref[...] = reduced(2, own[0], acc_fwd)
    for layer in range(2):
        @pl.loop(0, local_experts)
        def _(e):
            for copy in factor_copies(layer, e):
                copy.wait()
    for i, (source, target) in enumerate(kept):
        pltpu.make_async_copy(source, target, o_sem.at[i]).wait()
    wait(sent)
    dx_in_ref[...] = reduced(3, own[1], acc)
    wait(sent_dg)
    value = dg_send[...]
    for k in range(1, n):
        value += dg_recv[lax.rem(me + k, n)]
    value = pltpu.roll(value, lax.rem((n - me) * tok, rows), 1)
    dgate_a_ref[...] = value[0:top, 0:tok]
    dgate_b_ref[...] = value[PAD:PAD + top, 0:tok]


def grads_kernel(
    xa, xb, dya, dyb, ids_ref, gates_ref, h_ref, da_ref, db_ref, x_out_in, dx_in_in, dga_in, dgb_in,
    dw1_a, dw3_a, dw2_a, dw1_b, dw3_b, dw2_b, x_out, dx_in, dga, dgb,
):
    e = pl.program_id(0)
    expert = lax.axis_index("ep") * pl.num_programs(0) + e

    @pl.when(e == 0)
    def _():
        x_out[...] = x_out_in[...]
        dx_in[...] = dx_in_in[...]
        dga[...] = dga_in[...]
        dgb[...] = dgb_in[...]

    for layer, (x, dy, dw1, dw3, dw2) in enumerate(((xa, dya, dw1_a, dw3_a, dw2_a), (xb, dyb, dw1_b, dw3_b, dw2_b))):
        gate = jnp.sum(jnp.where(ids_ref[layer] == expert.astype(F32), gates_ref[layer], 0.0), axis=1, keepdims=True)
        q = (gate * dy[...].astype(F32)).astype(BF16)
        dw2[0] = mm(h_ref[layer, 0], q, TN)
        dw1[0] = mm(x[...], da_ref[layer, 0], TN)
        dw3[0] = mm(x[...], db_ref[layer, 0], TN)


def solution(mesh):
    n = mesh.shape["ep"]
    tok_spec = P(("dp", "ep"))
    w_spec = P("ep")

    def device_program(x_in, idx_a, idx_b, gate_a, gate_b, dy_out, w1_a, w3_a, w2_a, w1_b, w3_b, w2_b):
        tok, width = x_in.shape
        top = idx_a.shape[1]
        experts, _, ff = w1_a.shape
        rows = n * tok
        vmem = pl.BlockSpec(memory_space=pltpu.VMEM)
        anyw = pl.BlockSpec(memory_space=pl.ANY)
        sds = jax.ShapeDtypeStruct
        factor = sds((2, experts, rows, ff), BF16)
        gathered = sds((n, tok, width), BF16)
        tokens = pltpu.VMEM((n, tok, width), BF16)
        sums = pltpu.VMEM((n, tok, width), F32)
        outs = pl.pallas_call(
            functools.partial(step_kernel, n),
            out_shape=(
                sds((tok, width), BF16), sds((tok, width), BF16), sds((top, tok), F32), sds((top, tok), F32),
                gathered, gathered, gathered, gathered,
                sds((2, rows, LANES), F32), sds((2, rows, LANES), F32), factor, factor, factor),
            in_specs=[vmem] * 6 + [anyw] * 6,
            out_specs=(vmem,) * 4 + (anyw,) * 9,
            scratch_shapes=[
                pltpu.VMEM((2, experts, width, ff), BF16), pltpu.VMEM((2, experts, width, ff), BF16), pltpu.VMEM((2, experts, ff, width), BF16),
                pltpu.VMEM((2, experts, rows, ff), BF16), pltpu.VMEM((2, experts, rows, ff), BF16), pltpu.VMEM((2, experts, rows, ff), BF16),
                pltpu.VMEM((experts, rows, ff), BF16), pltpu.VMEM((experts, rows, ff), F32), pltpu.VMEM((experts, rows, ff), F32), pltpu.VMEM((experts, rows, ff), F32),
                pltpu.VMEM((4, PAD, LANES), F32), pltpu.VMEM((n, PAD, LANES), F32), pltpu.VMEM((PAD, LANES), F32), pltpu.VMEM((LANES, LANES), F32),
                pltpu.VMEM((2, rows, LANES), F32), pltpu.VMEM((2, rows, LANES), F32),
                tokens, tokens, tokens, tokens, tokens,
                sums, sums, pltpu.VMEM((4, n, tok, width), F32), pltpu.VMEM((2, tok, width), BF16),
                pltpu.VMEM((2, rows, LANES), F32), pltpu.VMEM((2 * PAD, LANES), F32), pltpu.VMEM((n, 2 * PAD, LANES), F32),
                pltpu.SemaphoreType.DMA((2, 3, experts)), pltpu.SemaphoreType.DMA((2, 3, experts)), pltpu.SemaphoreType.DMA((6,)),
                pltpu.SemaphoreType.DMA((11, n - 1)), pltpu.SemaphoreType.DMA((11, n - 1)),
            ],
            compiler_params=pltpu.CompilerParams(collective_id=0, has_side_effects=True, vmem_limit_bytes=56 << 20),
            name="moe_step",
        )(x_in, dy_out, idx_a.T, idx_b.T, gate_a.T, gate_b.T, w1_a, w3_a, w2_a, w1_b, w3_b, w2_b)
        x_out, dx_in, dga, dgb, xa, xb, dya, dyb, ids, gates, h, da, db = outs
        flat = lambda v: v.reshape(rows, width)
        whole = lambda v: pl.BlockSpec(v.shape, lambda e: (0,) * v.ndim)
        fac = pl.BlockSpec((2, 1, rows, ff), lambda e: (0, e, 0, 0))
        dw_up = pl.BlockSpec((1, width, ff), lambda e: (e, 0, 0))
        dw_down = pl.BlockSpec((1, ff, width), lambda e: (e, 0, 0))
        small = [flat(xa), flat(xb), flat(dya), flat(dyb), ids, gates]
        last = [x_out, dx_in, dga, dgb]
        up, down = sds((experts, width, ff), F32), sds((experts, ff, width), F32)
        res = pl.pallas_call(
            grads_kernel,
            grid=(experts,),
            out_shape=(up, up, down, up, up, down) + tuple(sds(v.shape, v.dtype) for v in last),
            in_specs=[whole(v) for v in small] + [fac] * 3 + [whole(v) for v in last],
            out_specs=(dw_up, dw_up, dw_down, dw_up, dw_up, dw_down) + tuple(whole(v) for v in last),
            compiler_params=pltpu.CompilerParams(dimension_semantics=("arbitrary",), vmem_limit_bytes=63 << 20),
            name="moe_grads",
        )(*small, h, da, db, *last)
        g = res[:6]
        x_out, dx_in, dga, dgb = res[6:]
        return (x_out, dx_in) + g + (dga.T, dgb.T)

    return jax.shard_map(device_program, mesh=mesh, in_specs=(tok_spec,) * 6 + (w_spec,) * 6, out_specs=(tok_spec,) * 10, check_vma=False)
```
